128 devices in a mesh: dp: 8 (over y_lo, x), tensor: 16 (over y_hi, z, core).
Axes of the slice: x: 4, y: 4 (y_hi: 2, y_lo: 2; y = y_hi * 2 + y_lo), z: 4, core: 2. Of those that a mesh axis runs over, the one named last changes fastest.
Arguments:
- saved_input: bfloat16 [1024, 8192], P(('dp', 'tensor')), may hold values from -8 to 8
- keep_bits: int32 [1024, 448], P(('dp', 'tensor')), may hold values from -2147483648 to 2147483646, as said below
- norm_gain: bfloat16 [8192], P('dp'), may hold values from 0.099609375 to 1.8984375
- gate_weight: bfloat16 [8192, 14336], P('dp', 'tensor'), may hold values from -0.0625 to 0.0625
- up_weight: bfloat16 [8192, 14336], P('dp', 'tensor'), may hold values from -0.0625 to 0.0625
- down_weight: bfloat16 [14336, 8192], P('tensor', 'dp'), may hold values from -0.046875 to 0.046875
Outputs:
- layer_out: bfloat16 [1024, 8192], P('tensor', 'dp')
- row_check: float32 [1024], P('tensor')
The draws below stay inside these ranges and needn't reach their ends.
Inputs may be any that keep to these rules, and one draw needn't show every extreme that they name: `keep_bits`: bit k of word w of a token is the keep bit of hidden unit 32 w + k.
All inputs are finite; a program needn't handle non-finite values.
Results may differ from the reference program's by a relative error of at most 0.017.
Values may be sent and summed in bfloat16 or wider, within the bound.
No kernel may reach another device: no remote copies, remote signals or barrier semaphores. Data moves between devices by JAX's collectives and lax.ppermute only.
A program may use at most 64 MiB of HBM per device.

```python
import jax
import jax.numpy as jnp
from jax import lax

D = 8192
FF = 14336
TOKENS = 1024
WORDS = 448


def draw_saved_input(key, part):
    keys = jax.random.split(jax.random.fold_in(key, 11), 2)
    base = jax.random.normal(keys[0], (TOKENS, D), jnp.float32)
    rough = jnp.exp(jax.random.uniform(keys[1], (1, D), jnp.float32, -0.35, 0.35))
    rising = jnp.exp(jnp.linspace(-0.55, 0.55, D, dtype=jnp.float32))[None, :]
    values = base * rough * rising
    return jnp.clip(values, -8.0, 8.0).astype(jnp.bfloat16)


def draw_keep_bits(key, part):
    return jax.random.randint(jax.random.fold_in(key, 23), (TOKENS, WORDS), -2147483648, 2147483647, jnp.int32)


def block_levels(own_key, shape, shards, low, high):
    def one(dim, parts):
        heights = jax.random.uniform(jax.random.fold_in(jax.random.fold_in(own_key, 6), dim), (parts,), jnp.float32, low / len(shards), high / len(shards))
        return jnp.repeat(jnp.exp(heights), shape[dim] // parts).reshape((-1,) + (1,) * (len(shape) - dim - 1))

    gain = one(*shards[0])
    for cut in shards[1:]:
        gain = gain * one(*cut)
    return gain


def scatter_about(stream_key, dims, deviation, most, cuts=(), kind=jnp.bfloat16):
    level = block_levels(stream_key, dims, cuts, -0.22, 0.18) if cuts else 1.0
    result = jax.random.normal(stream_key, dims, jnp.float32) * deviation * level
    return jnp.minimum(jnp.maximum(result, -most), most).astype(kind)


def setup_inputs(seed: int = 0) -> dict:
    arg_keys = jax.random.split(jax.random.key(seed), 7)
    return {
        "saved_input": draw_saved_input(jax.random.fold_in(arg_keys[6], 71), 0),
        "keep_bits": draw_keep_bits(jax.random.fold_in(arg_keys[6], 71), 0),
        "norm_gain": jnp.clip(1.0 + 0.18 * jax.random.normal(arg_keys[2], (D,), jnp.float32), 0.099609375, 1.8984375).astype(jnp.bfloat16),
        "gate_weight": scatter_about(arg_keys[3], (D, FF), D ** -0.5, 0.0625, ((0, 8), (1, 16))),
        "up_weight": scatter_about(arg_keys[4], (D, FF), D ** -0.5, 0.0625, ((0, 8), (1, 16))),
        "down_weight": scatter_about(arg_keys[5], (FF, D), FF ** -0.5, 0.046875, ((0, 16), (1, 8))),
    }


def reference(saved_input, keep_bits, norm_gain, gate_weight, up_weight, down_weight):
    widened = saved_input.astype(jnp.float32)
    inv_rms = lax.rsqrt(lax.optimization_barrier(jnp.sum(widened * widened, axis=1, keepdims=True)) / D + 1e-05)
    normed = (widened * inv_rms * norm_gain.astype(jnp.float32)).astype(jnp.bfloat16)
    gate = jnp.dot(normed, gate_weight, preferred_element_type=jnp.float32)
    up_sum = jnp.dot(normed, up_weight, preferred_element_type=jnp.float32)
    shifts = jnp.arange(32, dtype=jnp.int32)
    keep_mask = jnp.bitwise_and(jnp.right_shift(keep_bits[:, :, None], shifts[None, None, :]), 1)
    keep_mask = keep_mask.reshape(keep_bits.shape[0], -1)
    hidden = (jax.nn.silu(gate) * up_sum * (2.0 * keep_mask.astype(jnp.float32))).astype(jnp.bfloat16)
    layer_out = (widened + jnp.dot(hidden, down_weight, preferred_element_type=jnp.float32)).astype(jnp.bfloat16)
    widened_out = layer_out.astype(jnp.float32)
    row_check = lax.optimization_barrier(jnp.sum(widened_out * widened_out, axis=1)) / D
    return (layer_out, row_check)
```

```python
import jax
import jax.numpy as jnp
from jax import lax
from jax.sharding import Mesh
from jax.sharding import PartitionSpec as P

D = 8192
DP = ("yl", "x")
TENSOR = ("yh", "z", "c")
CHIPS = ("yl", "x", "yh", "z")
SWAP = ((0, 1), (1, 0))


def split3(value):
    hi = value.astype(jnp.bfloat16)
    rest = value - hi.astype(jnp.float32)
    mid = rest.astype(jnp.bfloat16)
    low = (rest - mid.astype(jnp.float32)).astype(jnp.bfloat16)
    return hi, mid, low


def on_device(saved_input, keep_bits, norm_gain, gate_weight, up_weight, down_weight):
    core = lax.axis_index("c")
    rows = saved_input.shape[0]
    width = gate_weight.shape[0]
    units = gate_weight.shape[1]
    dp_width = lax.axis_size(DP)
    chip_tensor = lax.axis_size(("yh", "z"))

    wide = saved_input.astype(jnp.float32)
    inv_rms = lax.rsqrt(jnp.sum(wide * wide, axis=1, keepdims=True) / D + 1e-05)
    lane = lax.broadcasted_iota(jnp.int32, (rows, 128), 1)
    hi, mid, low = split3(inv_rms)
    zero = jnp.zeros((), jnp.bfloat16)
    extra = jnp.where(lane == 0, hi, jnp.where(lane == 1, mid, jnp.where(lane == 2, low, zero)))
    slices = saved_input.reshape(rows, dp_width, width).transpose(1, 0, 2)
    block = jnp.concatenate((slices, jnp.broadcast_to(extra[None], (dp_width, rows, 128))), axis=2)
    block = jnp.broadcast_to(block[:, None], (dp_width, chip_tensor, rows, width + 128))
    block = block.reshape(dp_width * chip_tensor, rows, width + 128)
    mine = lax.all_to_all(block, CHIPS, 0, 0, tiled=True)
    other = lax.ppermute(mine, "c", SWAP)

    gain = norm_gain.astype(jnp.float32)[None, :]

    def normed_of(part):
        part = part.reshape(-1, width + 128).astype(jnp.float32)
        scale = part[:, width : width + 1] + part[:, width + 1 : width + 2] + part[:, width + 2 : width + 3]
        return (part[:, :width] * scale * gain).astype(jnp.bfloat16)

    def projected(part):
        normed = normed_of(part)
        g = jnp.dot(normed, gate_weight, preferred_element_type=jnp.float32).astype(jnp.bfloat16)
        u = jnp.dot(normed, up_weight, preferred_element_type=jnp.float32).astype(jnp.bfloat16)
        return jnp.concatenate((g, u), axis=1).reshape(dp_width, -1, 2 * units)

    a, b = projected(mine), projected(other)
    first = jnp.where(core == 0, a, b)
    second = jnp.where(core == 0, b, a)
    partial = jnp.concatenate((first, second), axis=1)
    arrived = lax.all_to_all(partial, DP, 0, 0, tiled=True)
    summed = jnp.sum(arrived.astype(jnp.float32), axis=0)

    words = lax.all_to_all(keep_bits, TENSOR, split_axis=1, concat_axis=0, tiled=True)
    words = words.reshape(chip_tensor, 2, rows, -1).transpose(1, 0, 2, 3).reshape(2 * chip_tensor * rows, -1)
    shifts = jnp.arange(32, dtype=jnp.int32)
    keep = jnp.bitwise_and(jnp.right_shift(words[:, :, None], shifts[None, None, :]), 1)
    keep = 2.0 * keep.reshape(words.shape[0], -1).astype(jnp.float32)
    hidden = (jax.nn.silu(summed[:, :units]) * summed[:, units:] * keep).astype(jnp.bfloat16)

    per_dp = hidden.shape[0]
    hidden = jnp.broadcast_to(hidden[None], (dp_width, *hidden.shape))
    hidden = lax.all_to_all(hidden, DP, 0, 0, tiled=True).reshape(-1, units)
    out = jnp.dot(hidden, down_weight, preferred_element_type=jnp.float32)
    out = out.astype(jnp.bfloat16).reshape(dp_width, 2, 2, -1, rows, width)
    keep_half = lax.dynamic_index_in_dim(out, core, 2, keepdims=False)
    send_half = lax.dynamic_index_in_dim(out, 1 - core, 2, keepdims=False)
    came = lax.ppermute(send_half, "c", SWAP)
    half = (keep_half.astype(jnp.float32) + came.astype(jnp.float32)).astype(jnp.bfloat16)
    half = half.transpose(0, 2, 1, 3, 4).reshape(dp_width, -1, width)
    parts = lax.all_to_all(half, ("yh", "z"), 0, 0, tiled=True)
    mlp = jnp.sum(parts.astype(jnp.float32), axis=0)

    own = lax.axis_index(("yh", "z"))

    def raw_rows(part):
        part = part.reshape(dp_width, 2, -1, rows, width + 128)
        part = lax.dynamic_index_in_dim(part, own, 0, keepdims=False)
        part = lax.dynamic_index_in_dim(part, core, 0, keepdims=False)
        return part[:, :, :width]

    r_mine, r_other = raw_rows(mine), raw_rows(other)
    residual = jnp.stack(
        (jnp.where(core == 0, r_mine, r_other), jnp.where(core == 0, r_other, r_mine)), axis=1
    ).reshape(-1, width)
    layer_out = (residual.astype(jnp.float32) + mlp).astype(jnp.bfloat16)
    w = layer_out.astype(jnp.float32)
    squares = jnp.sum(w * w, axis=1)
    every = lax.all_to_all(jnp.broadcast_to(squares[None], (dp_width, squares.shape[0])), DP, 0, 0, tiled=True)
    return layer_out, jnp.sum(every, axis=0) / D


def solution(mesh):
    torus = Mesh(mesh.devices.reshape(2, 4, 2, 4, 2), ("yl", "x", "yh", "z", "c"))
    return jax.shard_map(
        on_device,
        mesh=torus,
        in_specs=(
            P(DP + TENSOR, None),
            P(DP + TENSOR, None),
            P(DP),
            P(DP, TENSOR),
            P(DP, TENSOR),
            P(TENSOR, DP),
        ),
        out_specs=(P(TENSOR, DP), P(TENSOR)),
        check_vma=False,
    )
```

```python
import functools

import jax
import jax.numpy as jnp
from jax import lax
from jax.experimental import pallas as pl
from jax.experimental.pallas import tpu as pltpu
from jax.sharding import Mesh
from jax.sharding import PartitionSpec as P

D = 8192
DP = ("yl", "x")
TENSOR = ("yh", "z", "c")
CHIPS = ("yl", "x", "yh", "z")
SWAP = ((0, 1), (1, 0))
LINK = (("yl", SWAP), ("x", ((0, 3), (3, 0), (1, 2), (2, 1))), ("x", ((0, 1), (1, 0), (2, 3), (3, 2))))
STREAMS = (
    ((2, 1, 0), ((0, 0), (0, 1), (0, 2))),
    ((1, 0, 2), ((0, 3), (1, 0), (1, 1))),
    ((0, 2, 1), ((1, 2), (1, 3))),
)


def split3(value):
    hi = value.astype(jnp.bfloat16)
    rest = value - hi.astype(jnp.float32)
    mid = rest.astype(jnp.bfloat16)
    low = (rest - mid.astype(jnp.float32)).astype(jnp.bfloat16)
    return hi, mid, low


def cube_bits():
    x = lax.axis_index("x")
    return (lax.axis_index("yl"), x // 2, (x // 2) ^ (x % 2))


def added(keep, came):
    return keep.astype(jnp.float32) + came.astype(jnp.float32)


def sum_over_cube(keep, send, order):
    for step, dim in enumerate(order):
        axis, perm = LINK[dim]
        came = lax.ppermute(send, axis, perm)
        if step < 2:
            after = order[step + 1]
            near = [lax.slice_in_dim(v, 0, 1, axis=after) for v in (keep, came)]
            far = [lax.slice_in_dim(v, 1, 2, axis=after) for v in (keep, came)]
            send = added(*far).astype(jnp.bfloat16)
            keep = added(*near).astype(jnp.bfloat16)
    parts = added(keep, came)
    return parts.reshape(parts.shape[3:])


def gather_over_cube(block, order, masks):
    block = block[None, None, None]
    for dim in reversed(order):
        axis, perm = LINK[dim]
        came = lax.ppermute(block, axis, perm)
        upper = masks[dim, : block.shape[-1]] > 0.5
        block = jnp.where(
            upper, jnp.concatenate((came, block), axis=dim), jnp.concatenate((block, came), axis=dim)
        )
    return block


def cube_places():
    yl, x = lax.axis_index("yl"), lax.axis_index("x")
    places = []
    for r in range(8):
        p = 1 - yl if r & 4 else yl
        q = 3 - x if r & 2 else x
        places.append(p * 4 + (q ^ 1 if r & 1 else q))
    return jnp.stack(places).astype(jnp.int32)


def project(side, places_ref, mine_ref, other_ref, gain_ref, gate_ref, up_ref, *refs):
    out_refs, (normed_ref, gate_here, up_here, sems) = refs[:-4], refs[-4:]
    width, units = gate_ref.shape
    loads = [
        pltpu.make_async_copy(gate_ref, gate_here, sems.at[0]),
        pltpu.make_async_copy(up_ref, up_here, sems.at[1]),
    ]
    for load in loads:
        load.start()
    rows = mine_ref.shape[3]
    gain = gain_ref[...]
    at = 0
    spans = []
    for order, pieces in STREAMS:
        begin = at
        for r in range(8):
            if (r >> (2 - order[0])) & 1 != side:
                continue
            place = places_ref[r]
            for c, z in pieces:
                for yh in range(2):
                    value = (other_ref if c else mine_ref)[place, yh, z]
                    tail = value[:, width:].astype(jnp.float32)
                    scale = tail[:, 0:1] + tail[:, 1:2] + tail[:, 2:3]
                    normed_ref[at : at + rows] = (value[:, :width].astype(jnp.float32) * scale * gain).astype(jnp.bfloat16)
                    at += rows
        spans.append((begin, at))
    left = normed_ref[...]
    for base, ref, load in ((0, gate_here, loads[0]), (units, up_here, loads[1])):
        load.wait()
        for low in range(0, units, 256):
            high = min(low + 256, units)
            out = jnp.dot(left, ref[:, low:high], preferred_element_type=jnp.float32).astype(jnp.bfloat16)
            for (begin, end), out_ref in zip(spans, out_refs):
                out_ref[:, base + low : base + high] = out[begin:end]


def projected(side, places, mine, other, gain, gate_weight, up_weight):
    width, units = gate_weight.shape
    rows = mine.shape[3]
    vmem, smem = pl.BlockSpec(memory_space=pltpu.VMEM), pl.BlockSpec(memory_space=pltpu.SMEM)
    counts = [4 * 2 * len(pieces) * rows for _, pieces in STREAMS]
    outs = pl.pallas_call(
        functools.partial(project, side),
        out_shape=[jax.ShapeDtypeStruct((n, 2 * units), jnp.bfloat16) for n in counts],
        in_specs=[smem] + [vmem] * 3 + [pl.BlockSpec(memory_space=pl.ANY)] * 2,
        out_specs=[vmem] * len(counts),
        scratch_shapes=[
            pltpu.VMEM((sum(counts), width), jnp.bfloat16),
            pltpu.VMEM((width, units), jnp.bfloat16),
            pltpu.VMEM((width, units), jnp.bfloat16),
            pltpu.SemaphoreType.DMA((2,)),
        ],
        compiler_params=pltpu.CompilerParams(vmem_limit_bytes=20 * 2**20),
        cost_estimate=pl.CostEstimate(flops=4 * sum(counts) * width * units, bytes_accessed=8 * 2**20, transcendentals=0),
    )(places, mine, other, gain, gate_weight, up_weight)
    shaped = []
    for (order, pieces), out in zip(STREAMS, outs):
        shape = [2, 2, 2, out.shape[0] // 4, 2 * units]
        shape[order[0]] = 1
        shaped.append(out.reshape(shape))
    return shaped


def gray(blocks):
    return jnp.concatenate((blocks[:, :2], blocks[:, 3:], blocks[:, 2:3]), axis=1)


def on_device(saved_input, keep_bits, norm_gain, gate_weight, up_weight, down_weight):
    core = lax.axis_index("c")
    bits = cube_bits()
    rows = saved_input.shape[0]
    width = gate_weight.shape[0]
    units = gate_weight.shape[1]
    dp_width = lax.axis_size(DP)
    zs = lax.axis_size("z")
    chip_tensor = 2 * zs

    wide = saved_input.astype(jnp.float32)
    inv_rms = lax.rsqrt(jnp.sum(wide * wide, axis=1, keepdims=True) / D + 1e-05)
    lane = lax.broadcasted_iota(jnp.int32, (rows, 128), 1)
    hi, mid, low = split3(inv_rms)
    zero = jnp.zeros((), jnp.bfloat16)
    extra = jnp.where(lane == 0, hi, jnp.where(lane == 1, mid, jnp.where(lane == 2, low, zero)))
    slices = saved_input.reshape(rows, dp_width, width).transpose(1, 0, 2)
    block = jnp.concatenate((slices, jnp.broadcast_to(extra[None], (dp_width, rows, 128))), axis=2)
    block = jnp.broadcast_to(block[:, None], (dp_width, chip_tensor, rows, width + 128))
    block = block.reshape(dp_width * chip_tensor, rows, width + 128)
    masks = jnp.stack((*bits, core)).astype(jnp.float32)
    masks = jnp.broadcast_to(masks[:, None], (4, width))
    block, masks, places = lax.optimization_barrier((block, masks, cube_places()))
    second = masks[3] > 0.5
    mine = lax.all_to_all(block, CHIPS, 0, 0, tiled=True)
    other = lax.ppermute(mine, "c", SWAP)

    gain = norm_gain.astype(jnp.float32)[None, :]

    mine = mine.reshape(dp_width, 2, zs, rows, width + 128)
    other = other.reshape(mine.shape)
    sent = projected(1, places, mine, other, gain, gate_weight, up_weight)
    held = projected(0, places, mine, other, gain, gate_weight, up_weight)

    keep_bits, held[2] = lax.optimization_barrier((keep_bits, held[2]))
    words = lax.all_to_all(keep_bits, TENSOR, split_axis=1, concat_axis=0, tiled=True)
    words = words.reshape(2, zs, 2, rows, -1)
    words = jnp.where(second[: words.shape[-1]], words[:, :, ::-1], words)
    words = words.reshape(-1, words.shape[-1])
    count = words.shape[1]
    octets = jnp.concatenate([jnp.bitwise_and(jnp.right_shift(words, s), 255) for s in (0, 8, 16, 24)], axis=1)
    at = lax.broadcasted_iota(jnp.int32, (4 * count, units), 0)
    unit = lax.broadcasted_iota(jnp.int32, (4 * count, units), 1)
    pick = (at == (unit // 8) % 4 * count + unit // 32).astype(jnp.bfloat16)
    octet = jnp.dot(octets.astype(jnp.bfloat16), pick, preferred_element_type=jnp.float32).astype(jnp.int32)
    shift = lax.broadcasted_iota(jnp.int32, octet.shape, 1) % 8
    keep = 2.0 * jnp.bitwise_and(jnp.right_shift(octet, shift), 1).astype(jnp.float32)
    keep = keep.reshape(2, zs, 2, rows, units)

    kept, came = {}, {}
    for s, (order, pieces) in enumerate(STREAMS):
        summed = sum_over_cube(held[s], sent[s], order)
        scale = jnp.stack([keep[:, z, c] for c, z in pieces], axis=0).reshape(-1, units)
        hidden = (jax.nn.silu(summed[:, :units]) * summed[:, units:] * scale).astype(jnp.bfloat16)
        every = gather_over_cube(hidden, order, masks)
        out = jnp.dot(every.reshape(-1, units), down_weight, preferred_element_type=jnp.float32)
        out = out.astype(jnp.bfloat16).reshape(2, 4, len(pieces), 2, rows, width)
        mine_half = jnp.where(second, out[:, :, :, 1], out[:, :, :, 0])
        away = lax.ppermute(jnp.where(second, out[:, :, :, 0], out[:, :, :, 1]), "c", SWAP)
        for i, (c, z) in enumerate(pieces):
            kept[(c, z)] = mine_half[:, :, i]
            came[(1 - c, z)] = away[:, :, i]

    places = [(c, z) for c in range(2) for z in range(zs)]
    half = jnp.stack([kept[p] for p in places], axis=2).astype(jnp.float32)
    half = half + jnp.stack([came[p] for p in places], axis=2).astype(jnp.float32)
    half = gray(half.astype(jnp.bfloat16)).reshape(dp_width, -1, width)
    parts = lax.all_to_all(half, ("yh", "z"), 0, 0, tiled=True)
    return finish(parts, mine, other, core, second, dp_width, zs, rows, width)


def finish(parts, mine, other, core, second, dp_width, zs, rows, width):
    own = lax.axis_index(("yh", "z"))

    def raw_rows(part):
        part = part.reshape(dp_width, 2, zs, rows, width + 128)
        part = lax.dynamic_index_in_dim(part, own, 0, keepdims=False)
        part = lax.dynamic_index_in_dim(part, core, 0, keepdims=False)
        return part[:, :, :width]

    mlp = jnp.sum(parts.astype(jnp.float32), axis=0).reshape(2, zs, rows, width)
    raw = jnp.stack((raw_rows(mine), raw_rows(other)), axis=0)
    layer_out = (raw.astype(jnp.float32) + mlp).astype(jnp.bfloat16)
    layer_out = jnp.where(second, layer_out[::-1], layer_out)
    layer_out = layer_out.transpose(1, 0, 2, 3).reshape(-1, width)
    w = layer_out.astype(jnp.float32)
    squares = jnp.sum(w * w, axis=1)
    every = lax.all_to_all(jnp.broadcast_to(squares[None], (dp_width, squares.shape[0])), DP, 0, 0, tiled=True)
    return layer_out, jnp.sum(every, axis=0) / D


def solution(mesh):
    torus = Mesh(mesh.devices.reshape(2, 4, 2, 4, 2), ("yl", "x", "yh", "z", "c"))

    return jax.shard_map(
        on_device,
        mesh=torus,
        in_specs=(
            P(DP + TENSOR, None),
            P(DP + TENSOR, None),
            P(DP),
            P(DP, TENSOR),
            P(DP, TENSOR),
            P(TENSOR, DP),
        ),
        out_specs=(P(TENSOR, DP), P(TENSOR)),
        check_vma=False,
    )
```

```python
import functools

import jax
import jax.numpy as jnp
from jax import lax
from jax.experimental import pallas as pl
from jax.experimental.pallas import tpu as pltpu
from jax.sharding import Mesh
from jax.sharding import PartitionSpec as P

D = 8192
DP = ("yl", "x")
TENSOR = ("yh", "z", "c")
CHIPS = ("yl", "x", "yh", "z")
SWAP = ((0, 1), (1, 0))
LINK = (("yl", SWAP), ("x", ((0, 3), (3, 0), (1, 2), (2, 1))), ("x", ((0, 1), (1, 0), (2, 3), (3, 2))))
STREAMS = (
    ((2, 1, 0), ((0, 0), (0, 1), (0, 2))),
    ((1, 0, 2), ((0, 3), (1, 0), (1, 1))),
    ((0, 2, 1), ((1, 2), (1, 3))),
)


def leading(value):
    large = value * 65537.0
    return large - (large - value)


def pack(x_ref, words_ref, out_ref, wide_ref):
    rows, depth = x_ref.shape
    words = words_ref.shape[1]
    chips = out_ref.shape[0] // 8
    width = depth // 8
    each = words // chips
    total = jnp.zeros((rows, 1), jnp.float32)
    for low in range(0, depth, width):
        part = x_ref[:, low : low + width].astype(jnp.float32)
        total = total + jnp.sum(part * part, axis=1, keepdims=True)
    scale = lax.rsqrt(total / D + 1e-05)
    hi = leading(scale)
    mid = leading(scale - hi)
    low = scale - hi - mid
    wide_ref[...] = jnp.zeros_like(wide_ref)
    wide_ref[:, :words] = words_ref[...]
    span = wide_ref.shape[1]
    octets = [jnp.bitwise_and(jnp.right_shift(wide_ref[...], 8 * i), 255) for i in range(4)]
    lane = lax.broadcasted_iota(jnp.int32, (rows, TAIL), 1)
    for chip in range(chips):
        tail = jnp.zeros((rows, TAIL), jnp.int32)
        for i in range(4):
            moved = pltpu.roll(octets[i], (each * (i - chip)) % span, 1)[:, :TAIL]
            tail = jnp.where((lane >= each * i) & (lane < each * (i + 1)), moved, tail)
        tail = tail.astype(jnp.float32)
        for i, value in enumerate((hi, mid, low)):
            tail = jnp.where(lane == 4 * each + i, value, tail)
        tail = tail.astype(jnp.bfloat16)
        for dp in range(8):
            out_ref[dp * chips + chip, :, :width] = x_ref[:, dp * width : (dp + 1) * width]
            out_ref[dp * chips + chip, :, width:] = tail


def unpack(at_ref, mine_ref, other_ref, keep_ref, raw_ref, tail_ref):
    own, core, chip = at_ref[0], at_ref[8], at_ref[9]
    rows, width = raw_ref.shape[2:]
    units = keep_ref.shape[1]
    at = 0
    for _, pieces in STREAMS:
        for c, z in pieces:
            for yh in range(2):
                tail_ref[at : at + rows] = (other_ref if c else mine_ref)[own, yh, z][:, width:]
                at += rows
    lane = lax.broadcasted_iota(jnp.int32, (TAIL, units), 0)
    unit = lax.broadcasted_iota(jnp.int32, (TAIL, units), 1)
    count = units // 32
    pick = lane == jnp.bitwise_and(jnp.right_shift(unit, 3), 3) * (2 * count) + core * count + jnp.right_shift(unit, 5)
    pick = jnp.where(pick, 1.0, 0.0).astype(jnp.bfloat16)
    octet = jnp.dot(tail_ref[...], pick, preferred_element_type=jnp.float32).astype(jnp.int32)
    shift = jnp.bitwise_and(lax.broadcasted_iota(jnp.int32, octet.shape, 1), 7)
    keep_ref[...] = 2.0 * jnp.bitwise_and(jnp.right_shift(octet, shift), 1).astype(jnp.float32)
    for z in range(raw_ref.shape[0]):
        raw_ref[z, core] = mine_ref[chip, core, z][:, :width]
        raw_ref[z, 1 - core] = other_ref[chip, core, z][:, :width]


def packed(saved_input, keep_bits, width):
    rows = saved_input.shape[0]
    return pl.pallas_call(
        pack,
        out_shape=jax.ShapeDtypeStruct((64, rows, width + TAIL), jnp.bfloat16),
        in_specs=[pl.BlockSpec(memory_space=pltpu.VMEM)] * 2,
        out_specs=pl.BlockSpec(memory_space=pltpu.VMEM),
        scratch_shapes=[pltpu.VMEM((rows, 512), jnp.int32)],
        compiler_params=pltpu.CompilerParams(vmem_limit_bytes=8 * 2**20),
    )(saved_input, keep_bits)


def unpacked(places, mine, other, units):
    rows, width = mine.shape[3], mine.shape[4] - TAIL
    zs = mine.shape[2]
    vmem, smem = pl.BlockSpec(memory_space=pltpu.VMEM), pl.BlockSpec(memory_space=pltpu.SMEM)
    return pl.pallas_call(
        unpack,
        out_shape=[
            jax.ShapeDtypeStruct((4 * zs * rows, units), jnp.float32),
            jax.ShapeDtypeStruct((zs, 2, rows, width), jnp.bfloat16),
        ],
        in_specs=[smem, vmem, vmem],
        out_specs=[vmem, vmem],
        scratch_shapes=[pltpu.VMEM((4 * zs * rows, TAIL), jnp.bfloat16)],
        compiler_params=pltpu.CompilerParams(vmem_limit_bytes=12 * 2**20),
        cost_estimate=pl.CostEstimate(flops=10**7, bytes_accessed=10**6, transcendentals=0),
    )(places, mine, other)


def cube_bits():
    x = lax.axis_index("x")
    return (lax.axis_index("yl"), x // 2, (x // 2) ^ (x % 2))


TAIL = 256


def added(keep, came):
    return keep.astype(jnp.float32) + came.astype(jnp.float32)


def sum_over_cube(keep, send, order):
    for step, dim in enumerate(order):
        axis, perm = LINK[dim]
        came = lax.ppermute(send, axis, perm)
        if step < 2:
            after = order[step + 1]
            near = [lax.slice_in_dim(v, 0, 1, axis=after) for v in (keep, came)]
            far = [lax.slice_in_dim(v, 1, 2, axis=after) for v in (keep, came)]
            send = added(*far).astype(jnp.bfloat16)
            keep = added(*near).astype(jnp.bfloat16)
    parts = added(keep, came)
    return parts.reshape(parts.shape[3:])


def gather_over_cube(block, order, masks):
    block = block[None, None, None]
    for dim in reversed(order):
        axis, perm = LINK[dim]
        came = lax.ppermute(block, axis, perm)
        upper = masks[dim, : block.shape[-1]] > 0.5
        block = jnp.where(
            upper, jnp.concatenate((came, block), axis=dim), jnp.concatenate((block, came), axis=dim)
        )
    return block


def cube_places():
    yl, x = lax.axis_index("yl"), lax.axis_index("x")
    places = []
    for r in range(8):
        p = 1 - yl if r & 4 else yl
        q = 3 - x if r & 2 else x
        places.append(p * 4 + (q ^ 1 if r & 1 else q))
    chip = lax.axis_index("yh") * 4 + lax.axis_index("z")
    return jnp.stack((*places, lax.axis_index("c"), chip)).astype(jnp.int32)


def project(side, places_ref, mine_ref, other_ref, gain_ref, gate_ref, up_ref, *refs):
    out_refs, (normed_ref, gate_here, up_here, sems) = refs[:-4], refs[-4:]
    width, units = gate_ref.shape
    loads = [
        pltpu.make_async_copy(gate_ref, gate_here, sems.at[0]),
        pltpu.make_async_copy(up_ref, up_here, sems.at[1]),
    ]
    for load in loads:
        load.start()
    rows = mine_ref.shape[3]
    gain = gain_ref[...]
    at0 = units // 4
    at = 0
    spans = []
    for order, pieces in STREAMS:
        begin = at
        for r in range(8):
            if (r >> (2 - order[0])) & 1 != side:
                continue
            place = places_ref[r]
            for c, z in pieces:
                for yh in range(2):
                    value = (other_ref if c else mine_ref)[place, yh, z]
                    tail = value[:, width:].astype(jnp.float32)
                    scale = tail[:, at0 : at0 + 1] + tail[:, at0 + 1 : at0 + 2] + tail[:, at0 + 2 : at0 + 3]
                    normed_ref[at : at + rows] = (value[:, :width].astype(jnp.float32) * scale * gain).astype(jnp.bfloat16)
                    at += rows
        spans.append((begin, at))
    left = normed_ref[...]
    for base, ref, load in ((0, gate_here, loads[0]), (units, up_here, loads[1])):
        load.wait()
        for low in range(0, units, 256):
            high = min(low + 256, units)
            out = jnp.dot(left, ref[:, low:high], preferred_element_type=jnp.float32).astype(jnp.bfloat16)
            for (begin, end), out_ref in zip(spans, out_refs):
                out_ref[:, base + low : base + high] = out[begin:end]


def projected(side, places, mine, other, gain, gate_weight, up_weight):
    width, units = gate_weight.shape
    rows = mine.shape[3]
    vmem, smem = pl.BlockSpec(memory_space=pltpu.VMEM), pl.BlockSpec(memory_space=pltpu.SMEM)
    counts = [4 * 2 * len(pieces) * rows for _, pieces in STREAMS]
    outs = pl.pallas_call(
        functools.partial(project, side),
        out_shape=[jax.ShapeDtypeStruct((n, 2 * units), jnp.bfloat16) for n in counts],
        in_specs=[smem] + [vmem] * 3 + [pl.BlockSpec(memory_space=pl.ANY)] * 2,
        out_specs=[vmem] * len(counts),
        scratch_shapes=[
            pltpu.VMEM((sum(counts), width), jnp.bfloat16),
            pltpu.VMEM((width, units), jnp.bfloat16),
            pltpu.VMEM((width, units), jnp.bfloat16),
            pltpu.SemaphoreType.DMA((2,)),
        ],
        compiler_params=pltpu.CompilerParams(vmem_limit_bytes=20 * 2**20),
        cost_estimate=pl.CostEstimate(flops=4 * sum(counts) * width * units, bytes_accessed=8 * 2**20, transcendentals=0),
    )(places, mine, other, gain, gate_weight, up_weight)
    shaped = []
    for (order, pieces), out in zip(STREAMS, outs):
        shape = [2, 2, 2, out.shape[0] // 4, 2 * units]
        shape[order[0]] = 1
        shaped.append(out.reshape(shape))
    return shaped


def gray(blocks):
    return jnp.concatenate((blocks[:, :2], blocks[:, 3:], blocks[:, 2:3]), axis=1)


def on_device(saved_input, keep_bits, norm_gain, gate_weight, up_weight, down_weight):
    core = lax.axis_index("c")
    bits = cube_bits()
    rows = saved_input.shape[0]
    width = gate_weight.shape[0]
    units = gate_weight.shape[1]
    dp_width = lax.axis_size(DP)
    zs = lax.axis_size("z")

    block = packed(saved_input, keep_bits, width)
    masks = jnp.stack((*bits, core)).astype(jnp.float32)
    masks = jnp.broadcast_to(masks[:, None], (4, width))
    block, masks, places = lax.optimization_barrier((block, masks, cube_places()))
    second = masks[3] > 0.5
    mine = lax.all_to_all(block, CHIPS, 0, 0, tiled=True)
    other = lax.ppermute(mine, "c", SWAP)

    gain = norm_gain.astype(jnp.float32)[None, :]

    mine = mine.reshape(dp_width, 2, zs, rows, width + TAIL)
    other = other.reshape(mine.shape)
    sent = projected(1, places, mine, other, gain, gate_weight, up_weight)
    held = projected(0, places, mine, other, gain, gate_weight, up_weight)

    keep, raw = unpacked(places, mine, other, units)

    kept, came = {}, {}
    done = 0
    for s, (order, pieces) in enumerate(STREAMS):
        summed = sum_over_cube(held[s], sent[s], order)
        scale = keep[done : done + summed.shape[0]]
        done += summed.shape[0]
        hidden = (jax.nn.silu(summed[:, :units]) * summed[:, units:] * scale).astype(jnp.bfloat16)
        every = gather_over_cube(hidden, order, masks)
        out = jnp.dot(every.reshape(-1, units), down_weight, preferred_element_type=jnp.float32)
        out = out.astype(jnp.bfloat16).reshape(2, 4, len(pieces), 2, rows, width)
        mine_half = jnp.where(second, out[:, :, :, 1], out[:, :, :, 0])
        away = lax.ppermute(jnp.where(second, out[:, :, :, 0], out[:, :, :, 1]), "c", SWAP)
        for i, (c, z) in enumerate(pieces):
            kept[(c, z)] = mine_half[:, :, i]
            came[(1 - c, z)] = away[:, :, i]

    places = [(c, z) for c in range(2) for z in range(zs)]
    half = jnp.stack([kept[p] for p in places], axis=2).astype(jnp.float32)
    half = half + jnp.stack([came[p] for p in places], axis=2).astype(jnp.float32)
    half = gray(half.astype(jnp.bfloat16)).reshape(dp_width, -1, width)
    parts = lax.all_to_all(half, ("yh", "z"), 0, 0, tiled=True)
    mlp = jnp.sum(parts.astype(jnp.float32), axis=0).reshape(2, zs, rows, width).transpose(1, 0, 2, 3)
    mlp = jnp.where(second, mlp[:, ::-1], mlp)
    layer_out = (raw.astype(jnp.float32) + mlp).astype(jnp.bfloat16).reshape(-1, width)
    w = layer_out.astype(jnp.float32)
    squares = jnp.sum(w * w, axis=1)
    every = lax.all_to_all(jnp.broadcast_to(squares[None], (dp_width, squares.shape[0])), DP, 0, 0, tiled=True)
    return layer_out, jnp.sum(every, axis=0) / D


def solution(mesh):
    torus = Mesh(mesh.devices.reshape(2, 4, 2, 4, 2), ("yl", "x", "yh", "z", "c"))

    return jax.shard_map(
        on_device,
        mesh=torus,
        in_specs=(
            P(DP + TENSOR, None),
            P(DP + TENSOR, None),
            P(DP),
            P(DP, TENSOR),
            P(DP, TENSOR),
            P(TENSOR, DP),
        ),
        out_specs=(P(TENSOR, DP), P(TENSOR)),
        check_vma=False,
    )
```

```python
import functools

import jax
import jax.numpy as jnp
from jax import lax
from jax.experimental import pallas as pl
from jax.experimental.pallas import tpu as pltpu
from jax.sharding import Mesh
from jax.sharding import PartitionSpec as P

D = 8192
DP = ("yl", "x")
TENSOR = ("yh", "z", "c")
CHIPS = ("yl", "x", "yh", "z")
SWAP = ((0, 1), (1, 0))
LINK = (("yl", SWAP), ("x", ((0, 3), (3, 0), (1, 2), (2, 1))), ("x", ((0, 1), (1, 0), (2, 3), (3, 2))))
STREAMS = (
    ((2, 1, 0), ((0, 0, 0), (0, 1, 0), (0, 0, 1), (0, 1, 1), (0, 0, 2), (0, 1, 2))),
    ((1, 0, 2), ((1, 0, 0), (1, 1, 0), (1, 0, 1), (1, 1, 1), (1, 0, 2))),
    ((0, 2, 1), ((1, 1, 2), (0, 0, 3), (0, 1, 3), (1, 0, 3), (1, 1, 3))),
)


def leading(value):
    large = value * 65537.0
    return large - (large - value)


def pack(x_far, words_far, out_ref, x_ref, wide_ref, words_ref, sems):
    loads = [pltpu.make_async_copy(x_far, x_ref, sems.at[0]), pltpu.make_async_copy(words_far, words_ref, sems.at[1])]
    for load in loads:
        load.start()
    for load in loads:
        load.wait()
    rows, depth = x_ref.shape
    words = words_ref.shape[1]
    chips = out_ref.shape[0] // 8
    width = depth // 8
    each = words // chips
    total = jnp.zeros((rows, 1), jnp.float32)
    for low in range(0, depth, width):
        part = x_ref[:, low : low + width].astype(jnp.float32)
        total = total + jnp.sum(part * part, axis=1, keepdims=True)
    scale = lax.rsqrt(total / D + 1e-05)
    hi = leading(scale)
    mid = leading(scale - hi)
    low = scale - hi - mid
    wide_ref[...] = jnp.zeros_like(wide_ref)
    wide_ref[:, :words] = words_ref[...]
    span = wide_ref.shape[1]
    octets = [jnp.bitwise_and(jnp.right_shift(wide_ref[...], 8 * i), 255) for i in range(4)]
    lane = lax.broadcasted_iota(jnp.int32, (rows, TAIL), 1)
    for chip in range(chips):
        tail = jnp.zeros((rows, TAIL), jnp.int32)
        for i in range(4):
            moved = pltpu.roll(octets[i], (each * (i - chip)) % span, 1)[:, :TAIL]
            tail = jnp.where((lane >= each * i) & (lane < each * (i + 1)), moved, tail)
        tail = tail.astype(jnp.float32)
        for i, value in enumerate((hi, mid, low)):
            tail = jnp.where(lane == 4 * each + i, value, tail)
        tail = tail.astype(jnp.bfloat16)
        for dp in range(8):
            out_ref[dp * chips + chip, :, :width] = x_ref[:, dp * width : (dp + 1) * width]
            out_ref[dp * chips + chip, :, width:] = tail


def unpack(at_ref, mine_ref, other_ref, keep_ref, raw_ref, tail_ref):
    core, chip = at_ref[8], at_ref[9]
    rows, width = raw_ref.shape[2:]
    units = keep_ref.shape[1]
    at = 0
    for order, pieces in STREAMS:
        dim = order[2]
        for half in range(2):
            place = at_ref[jnp.bitwise_xor(half, at_ref[10 + dim]) * (4 >> dim)]
            for c, yh, z in pieces:
                tail_ref[at : at + rows] = (other_ref if c else mine_ref)[place, yh, z][:, width:]
                at += rows
    lane = lax.broadcasted_iota(jnp.int32, (TAIL, units), 0)
    unit = lax.broadcasted_iota(jnp.int32, (TAIL, units), 1)
    count = units // 32
    pick = lane == jnp.bitwise_and(jnp.right_shift(unit, 3), 3) * (2 * count) + core * count + jnp.right_shift(unit, 5)
    pick = jnp.where(pick, 1.0, 0.0).astype(jnp.bfloat16)
    octet = jnp.dot(tail_ref[...], pick, preferred_element_type=jnp.float32).astype(jnp.int32)
    shift = jnp.bitwise_and(lax.broadcasted_iota(jnp.int32, octet.shape, 1), 7)
    keep_ref[...] = 2.0 * jnp.bitwise_and(jnp.right_shift(octet, shift), 1).astype(jnp.float32)
    for z in range(raw_ref.shape[0]):
        raw_ref[z, core] = mine_ref[chip, core, z][:, :width]
        raw_ref[z, 1 - core] = other_ref[chip, core, z][:, :width]


def packed(saved_input, keep_bits, width):
    rows = saved_input.shape[0]
    return pl.pallas_call(
        pack,
        out_shape=jax.ShapeDtypeStruct((64, rows, width + TAIL), jnp.bfloat16),
        in_specs=[pl.BlockSpec(memory_space=pltpu.HBM)] * 2,
        out_specs=pl.BlockSpec(memory_space=pltpu.VMEM),
        scratch_shapes=[
            pltpu.VMEM(saved_input.shape, jnp.bfloat16),
            pltpu.VMEM((rows, 512), jnp.int32),
            pltpu.VMEM(keep_bits.shape, jnp.int32),
            pltpu.SemaphoreType.DMA((2,)),
        ],
        compiler_params=pltpu.CompilerParams(vmem_limit_bytes=8 * 2**20),
    )(saved_input, keep_bits)


def unpacked(places, mine, other, units):
    rows, width = mine.shape[3], mine.shape[4] - TAIL
    zs = mine.shape[2]
    vmem, smem = pl.BlockSpec(memory_space=pltpu.VMEM), pl.BlockSpec(memory_space=pltpu.SMEM)
    return pl.pallas_call(
        unpack,
        out_shape=[
            jax.ShapeDtypeStruct((8 * zs * rows, units), jnp.float32),
            jax.ShapeDtypeStruct((zs, 2, rows, width), jnp.bfloat16),
        ],
        in_specs=[smem, vmem, vmem],
        out_specs=[vmem, vmem],
        scratch_shapes=[pltpu.VMEM((8 * zs * rows, TAIL), jnp.bfloat16)],
        compiler_params=pltpu.CompilerParams(vmem_limit_bytes=12 * 2**20),
        cost_estimate=pl.CostEstimate(flops=10**7, bytes_accessed=10**6, transcendentals=0),
    )(places, mine, other)


def cube_bits():
    x = lax.axis_index("x")
    return (lax.axis_index("yl"), x // 2, (x // 2) ^ (x % 2))


TAIL = 256


def added(keep, came):
    return keep.astype(jnp.float32) + came.astype(jnp.float32)


def sum_over_cube(keep, send, order, masks):
    for step in range(2):
        axis, perm = LINK[order[step]]
        came = lax.ppermute(send, axis, perm)
        after = order[1]
        if step == 0:
            near = [lax.slice_in_dim(v, 0, 1, axis=after) for v in (keep, came)]
            far = [lax.slice_in_dim(v, 1, 2, axis=after) for v in (keep, came)]
            send = added(*far).astype(jnp.bfloat16)
            keep = added(*near).astype(jnp.bfloat16)
    dim = order[2]
    axis, perm = LINK[dim]
    low = [lax.slice_in_dim(v, 0, 1, axis=dim) for v in (keep, came)]
    high = [lax.slice_in_dim(v, 1, 2, axis=dim) for v in (keep, came)]
    upper = masks[dim, : keep.shape[-1] // 2] > 0.5
    upper = jnp.concatenate((upper, upper))
    low, high = added(*low), added(*high)
    both = jnp.concatenate((jnp.where(upper, high, low), jnp.where(upper, low, high)), axis=dim).astype(jnp.bfloat16)
    came = lax.ppermute(both, axis, perm)
    return added(both, came)


def gather_over_cube(block, order, masks):
    for dim in (order[1], order[0]):
        axis, perm = LINK[dim]
        came = lax.ppermute(block, axis, perm)
        upper = masks[dim, : block.shape[-1]] > 0.5
        block = jnp.where(
            upper, jnp.concatenate((came, block), axis=dim), jnp.concatenate((block, came), axis=dim)
        )
    return block


def cube_places():
    yl, x = lax.axis_index("yl"), lax.axis_index("x")
    places = []
    for r in range(8):
        p = 1 - yl if r & 4 else yl
        q = 3 - x if r & 2 else x
        places.append(p * 4 + (q ^ 1 if r & 1 else q))
    chip = lax.axis_index("yh") * 4 + lax.axis_index("z")
    return jnp.stack((*places, lax.axis_index("c"), chip, *cube_bits())).astype(jnp.int32)


def project(chosen, side, places_ref, mine_ref, other_ref, gain_ref, gate_ref, up_ref, *refs):
    out_refs, (normed_ref, gate_here, up_here, sems) = refs[:-4], refs[-4:]
    width, units = gate_ref.shape
    loads = [
        pltpu.make_async_copy(gate_ref, gate_here, sems.at[0]),
        pltpu.make_async_copy(up_ref, up_here, sems.at[1]),
    ]
    for load in loads:
        load.start()
    rows = mine_ref.shape[3]
    gain = gain_ref[...]
    at0 = units // 4
    at = 0
    spans = []
    for order, pieces in chosen:
        begin = at
        for r in range(8):
            if (r >> (2 - order[0])) & 1 != side:
                continue
            place = places_ref[r]
            for c, yh, z in pieces:
                value = (other_ref if c else mine_ref)[place, yh, z]
                tail = value[:, width:].astype(jnp.float32)
                scale = tail[:, at0 : at0 + 1] + tail[:, at0 + 1 : at0 + 2] + tail[:, at0 + 2 : at0 + 3]
                normed_ref[at : at + rows] = (value[:, :width].astype(jnp.float32) * scale * gain).astype(jnp.bfloat16)
                at += rows
        spans.append((begin, at))
    left = normed_ref[...]
    for base, ref, load in ((0, gate_here, loads[0]), (units, up_here, loads[1])):
        load.wait()
        for low in range(0, units, 256):
            high = min(low + 256, units)
            out = jnp.dot(left, ref[:, low:high], preferred_element_type=jnp.float32).astype(jnp.bfloat16)
            for (begin, end), out_ref in zip(spans, out_refs):
                out_ref[:, base + low : base + high] = out[begin:end]


def projected(chosen, side, places, mine, other, gain, gate_weight, up_weight):
    width, units = gate_weight.shape
    rows = mine.shape[3]
    vmem, smem = pl.BlockSpec(memory_space=pltpu.VMEM), pl.BlockSpec(memory_space=pltpu.SMEM)
    counts = [4 * len(pieces) * rows for _, pieces in chosen]
    outs = pl.pallas_call(
        functools.partial(project, chosen, side),
        out_shape=[jax.ShapeDtypeStruct((n, 2 * units), jnp.bfloat16) for n in counts],
        in_specs=[smem] + [vmem] * 3 + [pl.BlockSpec(memory_space=pltpu.HBM)] * 2,
        out_specs=[vmem] * len(counts),
        scratch_shapes=[
            pltpu.VMEM((sum(counts), width), jnp.bfloat16),
            pltpu.VMEM((width, units), jnp.bfloat16),
            pltpu.VMEM((width, units), jnp.bfloat16),
            pltpu.SemaphoreType.DMA((2,)),
        ],
        compiler_params=pltpu.CompilerParams(vmem_limit_bytes=20 * 2**20),
        cost_estimate=pl.CostEstimate(flops=4 * sum(counts) * width * units, bytes_accessed=8 * 2**20, transcendentals=0),
    )(places, mine, other, gain, gate_weight, up_weight)
    shaped = []
    for (order, pieces), out in zip(chosen, outs):
        shape = [2, 2, 2, out.shape[0] // 4, 2 * units]
        shape[order[0]] = 1
        shaped.append(out.reshape(shape))
    return shaped


def gray(blocks):
    return jnp.concatenate((blocks[:, :2], blocks[:, 3:], blocks[:, 2:3]), axis=1)


def on_device(saved_input, keep_bits, norm_gain, gate_weight, up_weight, down_weight):
    core = lax.axis_index("c")
    bits = cube_bits()
    rows = saved_input.shape[0]
    width = gate_weight.shape[0]
    units = gate_weight.shape[1]
    dp_width = lax.axis_size(DP)
    zs = lax.axis_size("z")

    stay = functools.partial(pltpu.with_memory_space_constraint, memory_space=pltpu.HBM)
    gate_weight, up_weight = stay(gate_weight), stay(up_weight)
    block = packed(stay(saved_input), stay(keep_bits), width)
    masks = jnp.stack((*bits, core)).astype(jnp.float32)
    masks = jnp.broadcast_to(masks[:, None], (4, width))
    block, masks, places = lax.optimization_barrier((block, masks, cube_places()))
    second = masks[3] > 0.5
    mine = lax.all_to_all(block, CHIPS, 0, 0, tiled=True)
    other = lax.ppermute(mine, "c", SWAP)

    gain = norm_gain.astype(jnp.float32)[None, :]

    mine = mine.reshape(dp_width, 2, zs, rows, width + TAIL)
    other = other.reshape(mine.shape)
    sent = projected(STREAMS[:1], 1, places, mine, mine, gain, gate_weight, up_weight)
    sent += projected(STREAMS[1:], 1, places, mine, other, gain, gate_weight, up_weight)
    held = projected(STREAMS, 0, places, mine, other, gain, gate_weight, up_weight)

    keep, raw = unpacked(places, mine, other, units)

    blocks, kept, came = {}, {}, {}
    done = 0
    for s, (order, pieces) in enumerate(STREAMS):
        summed = sum_over_cube(held[s], sent[s], order, masks)
        scale = keep[done : done + 2 * rows * len(pieces)].reshape(*summed.shape[:-1], units)
        done += 2 * rows * len(pieces)
        hidden = (jax.nn.silu(summed[..., :units]) * summed[..., units:] * scale).astype(jnp.bfloat16)
        every = gather_over_cube(hidden, order, masks)
        out = jnp.dot(every.reshape(-1, units), down_weight, preferred_element_type=jnp.float32)
        out = out.astype(jnp.bfloat16).reshape(2, 4, len(pieces), rows, width)
        for i, piece in enumerate(pieces):
            blocks[piece] = out[:, :, i]
        ready = [(c, z) for c in range(2) for z in range(zs) if (c, z) not in kept and {(c, 0, z), (c, 1, z)} <= set(blocks)]
        if s == 1:
            continue
        pairs = [jnp.stack([blocks[(c, yh, z)] for c, z in ready], axis=2) for yh in range(2)]
        mine_half = jnp.where(second, pairs[1], pairs[0])
        away = lax.ppermute(jnp.where(second, pairs[0], pairs[1]), "c", SWAP)
        for i, (c, z) in enumerate(ready):
            kept[(c, z)] = mine_half[:, :, i]
            came[(1 - c, z)] = away[:, :, i]

    places = [(c, z) for c in range(2) for z in range(zs)]
    half = jnp.stack([kept[p] for p in places], axis=2).astype(jnp.float32)
    half = half + jnp.stack([came[p] for p in places], axis=2).astype(jnp.float32)
    half = gray(half.astype(jnp.bfloat16)).reshape(dp_width, -1, width)
    parts = lax.all_to_all(half, ("yh", "z"), 0, 0, tiled=True)
    mlp = jnp.sum(parts.astype(jnp.float32), axis=0).reshape(2, zs, rows, width).transpose(1, 0, 2, 3)
    mlp = jnp.where(second, mlp[:, ::-1], mlp)
    layer_out = (raw.astype(jnp.float32) + mlp).astype(jnp.bfloat16).reshape(-1, width)
    w = layer_out.astype(jnp.float32)
    squares = jnp.sum(w * w, axis=1)
    every = lax.all_to_all(jnp.broadcast_to(squares[None], (dp_width, squares.shape[0])), DP, 0, 0, tiled=True)
    return layer_out, jnp.sum(every, axis=0) / D


def solution(mesh):
    torus = Mesh(mesh.devices.reshape(2, 4, 2, 4, 2), ("yl", "x", "yh", "z", "c"))

    return jax.shard_map(
        on_device,
        mesh=torus,
        in_specs=(
            P(DP + TENSOR, None),
            P(DP + TENSOR, None),
            P(DP),
            P(DP, TENSOR),
            P(DP, TENSOR),
            P(TENSOR, DP),
        ),
        out_specs=(P(TENSOR, DP), P(TENSOR)),
        check_vma=False,
    )
```
